32 devices in a mesh: dp: 8 (over z, x), tensor: 4 (over y, core).
Axes of the slice: x: 2, y: 2, z: 4, core: 2. Of those that a mesh axis runs over, the one named last changes fastest.
Arguments:
- samples: bfloat16 [256, 64], P('dp'), may hold values from -6 to 6
- projections: bfloat16 [256, 256], P('dp'), may hold values from -6 to 6
- weight_in: bfloat16 [64, 2048], P(None, 'tensor'), may hold values from -0.75 to 0.75
- bias_in: bfloat16 [2048], P('tensor'), may hold values from -3 to 3
- weight_mid: bfloat16 [2048, 2048], P('tensor'), may hold values from -0.125 to 0.125
- bias_mid: bfloat16 [2048], replicated, may hold values from -3 to 3
- weight_out: bfloat16 [2048, 64], replicated, may hold values from -0.125 to 0.125
- bias_out: float32 [64], replicated, may hold values from -3 to 3
Outputs:
- sample_loss: float32 [256], P('dp')
- grad_weight_in: float32 [64, 2048], P(None, 'tensor')
- grad_bias_in: float32 [2048], P('tensor')
- grad_weight_mid: float32 [2048, 2048], P(('tensor', 'dp'))
- grad_bias_mid: float32 [2048], P('tensor')
- grad_weight_out: float32 [2048, 64], P('tensor')
- grad_bias_out: float32 [64], replicated
The draws below stay inside these ranges and needn't reach their ends.
All inputs are finite; a program needn't handle non-finite values.
Results may differ from the reference program's by a relative error of at most 0.01.
Values may be sent and summed in bfloat16 or wider, within the bound.
No kernel may reach another device: no remote copies, remote signals or barrier semaphores. Data moves between devices by JAX's collectives and lax.ppermute only.
A program may use at most 64 MiB of HBM per device.

```python
import jax
import jax.numpy as jnp
from jax import lax

D = 2048
P_SIZE = 64
M = 4
B_DEV = 32
NS = 256
N_DP = 8


def block_scale(key, shape, split, low, high):
    level = 1.0
    for position, blocks in split:
        steps = jax.random.uniform(jax.random.fold_in(jax.random.fold_in(key, 6), position), (blocks,), jnp.float32, low / len(split), high / len(split))
        level = level * jnp.repeat(jnp.exp(steps), shape[position] // blocks).reshape((-1,) + (1,) * (len(shape) - 1 - position))
    return level


def bell_draw(key, dims, width, bound, cuts=(), dtype=jnp.bfloat16):
    gain = block_scale(key, dims, cuts, -0.22, 0.18) if cuts else 1.0
    array = jax.random.normal(key, dims, jnp.float32) * width * gain
    return jnp.minimum(jnp.maximum(array, -bound), bound).astype(dtype)


def setup_inputs(seed: int = 0) -> dict:
    splits = jax.random.split(jax.random.key(seed), 9)
    return {
        "samples": bell_draw(splits[0], (NS, P_SIZE), 1.0, 6.0, ((0, 8),)),
        "projections": bell_draw(splits[1], (NS, M * P_SIZE), 1.0, 6.0, ((0, 8),)),
        "weight_in": bell_draw(splits[2], (P_SIZE, D), P_SIZE ** -0.5, 0.75, ((1, 4),)),
        "bias_in": bell_draw(splits[3], (D,), 0.5, 3.0, ((0, 4),)),
        "weight_mid": bell_draw(splits[4], (D, D), D ** -0.5, 0.125, ((0, 4),)),
        "bias_mid": bell_draw(splits[5], (D,), 0.5, 3.0),
        "weight_out": bell_draw(splits[6], (D, P_SIZE), D ** -0.5, 0.125),
        "bias_out": bell_draw(splits[7], (P_SIZE,), 0.5, 3.0, (), jnp.float32),
    }


row_contract = (((0,), (0,)), ((), ()))
col_contract = (((1,), (1,)), ((), ()))


def swish_layer(pre_act, tangent):
    logistic = jax.nn.sigmoid(pre_act)
    slopes = logistic * (1.0 + pre_act * (1.0 - logistic))
    curvature = logistic * (1.0 - logistic) * (2.0 + pre_act * (1.0 - 2.0 * logistic))
    active = (pre_act * logistic).astype(jnp.bfloat16)
    moved = (slopes[:, None, :] * tangent).astype(jnp.bfloat16)
    return active, moved, slopes, curvature


def swish_back(back_act, back_tan, tangent, slopes, curvature):
    grad_pre = back_act * slopes + curvature * jnp.sum(back_tan * tangent, axis=1)
    grad_tan = back_tan * slopes[:, None, :]
    return grad_pre, grad_tan


def stack_rows(head, tail):
    return jnp.concatenate([head, tail.reshape(-1, tail.shape[-1])], axis=0)


def reference(samples, projections, weight_in, bias_in, weight_mid, bias_mid, weight_out, bias_out):
    def block_step(carry, block_inputs):
        block_x, block_proj = block_inputs
        batch_rows = block_x.shape[0]
        vectors = block_proj.reshape(batch_rows * M, P_SIZE)
        directions = vectors.reshape(batch_rows, M, P_SIZE).astype(jnp.float32)
        inputs = jnp.concatenate([block_x, vectors], axis=0)
        pre_first = jnp.dot(inputs, weight_in, preferred_element_type=jnp.float32)
        hidden_in = pre_first[:batch_rows] + bias_in.astype(jnp.float32)
        tan_in = pre_first[batch_rows:].reshape(batch_rows, M, D)
        act_in, moved_in, slopes_in, curv_in = swish_layer(hidden_in, tan_in)
        layer_one = stack_rows(act_in, moved_in)
        pre_second = jnp.dot(layer_one, weight_mid, preferred_element_type=jnp.float32)
        hidden_mid = pre_second[:batch_rows] + bias_mid.astype(jnp.float32)
        tan_mid = pre_second[batch_rows:].reshape(batch_rows, M, D)
        act_mid, moved_mid, slopes_mid, curv_mid = swish_layer(hidden_mid, tan_mid)
        layer_two = stack_rows(act_mid, moved_mid)
        outputs = jnp.dot(layer_two, weight_out, preferred_element_type=jnp.float32)
        score = outputs[:batch_rows] + bias_out
        dscore = outputs[batch_rows:].reshape(batch_rows, M, P_SIZE)
        projected = jnp.sum(directions * score[:, None, :], axis=-1)
        traced = jnp.sum(directions * dscore, axis=-1)
        losses = jnp.mean(traced + 0.5 * projected * projected, axis=1)
        grad_score = jnp.einsum('bm,bmp->bp', projected, directions)
        score_low = grad_score.astype(jnp.bfloat16)
        out_rows = jnp.concatenate([score_low, vectors], axis=0)
        back_out = lax.dot_general(out_rows, weight_out, col_contract, preferred_element_type=jnp.float32)
        pre_mid_grad, tan_mid_grad = swish_back(back_out[:batch_rows], back_out[batch_rows:].reshape(batch_rows, M, D), tan_mid, slopes_mid, curv_mid)
        signal_mid = stack_rows(pre_mid_grad.astype(jnp.bfloat16), tan_mid_grad.astype(jnp.bfloat16))
        out_grad = lax.dot_general(layer_two, out_rows, row_contract, preferred_element_type=jnp.float32)
        mid_grad = lax.dot_general(layer_one, signal_mid, row_contract, preferred_element_type=jnp.float32)
        back_first = lax.dot_general(signal_mid, weight_mid, col_contract, preferred_element_type=jnp.float32)
        pre_in_grad, tan_in_grad = swish_back(back_first[:batch_rows], back_first[batch_rows:].reshape(batch_rows, M, D), tan_in, slopes_in, curv_in)
        signal_in = stack_rows(pre_in_grad.astype(jnp.bfloat16), tan_in_grad.astype(jnp.bfloat16))
        in_grad = lax.dot_general(inputs, signal_in, row_contract, preferred_element_type=jnp.float32)
        grads = (in_grad, jnp.sum(pre_in_grad, axis=0), mid_grad, jnp.sum(pre_mid_grad, axis=0), out_grad, jnp.sum(grad_score, axis=0))
        return tuple(old + new for old, new in zip(carry, grads)), losses

    init = (jnp.zeros((P_SIZE, D), jnp.float32), jnp.zeros((D,), jnp.float32), jnp.zeros((D, D), jnp.float32), jnp.zeros((D,), jnp.float32), jnp.zeros((D, P_SIZE), jnp.float32), jnp.zeros((P_SIZE,), jnp.float32))
    blocks_x = samples.reshape(N_DP, B_DEV, P_SIZE)
    blocks_p = projections.reshape(N_DP, B_DEV, M * P_SIZE)
    totals, losses = lax.scan(block_step, init, (blocks_x, blocks_p))
    scale_factor = 1.0 / (NS * M)
    return (losses.reshape(NS), totals[0] * scale_factor, totals[1] * scale_factor, totals[2] * scale_factor, totals[3] * scale_factor, totals[4] * scale_factor, totals[5] * scale_factor)
```

```python
import jax
import jax.numpy as jnp
from jax import lax
from jax.experimental import pallas as pl
from jax.experimental.pallas import tpu as pltpu
from jax.sharding import PartitionSpec as P


F32 = jnp.float32
BF16 = jnp.bfloat16
NN = (((1,), (0,)), ((), ()))
NT = (((1,), (1,)), ((), ()))
TN = (((0,), (0,)), ((), ()))


def mm(a, b, dims):
    return lax.dot_general(a, b, dims, preferred_element_type=F32)


def stack(parts):
    return jnp.concatenate(parts, axis=0)


def swish_terms(hidden):
    gate = jax.nn.sigmoid(hidden)
    slopes = gate * (1.0 + hidden * (1.0 - gate))
    curv = gate * (1.0 - gate) * (2.0 + hidden * (1.0 - 2.0 * gate))
    return hidden * gate, slopes, curv


def rows_of(full, rows):
    count = full.shape[0] // rows
    return [full[i * rows : (i + 1) * rows] for i in range(count)]


def packed_rows(packed, patch):
    count = packed.shape[1] // patch
    return stack([packed[:, i * patch : (i + 1) * patch] for i in range(count)])


def forward_layer(pieces, bias):
    act, slopes, curv = swish_terms(pieces[0] + bias)
    layer = stack([act.astype(BF16)] + [(slopes * tan).astype(BF16) for tan in pieces[1:]])
    return layer, slopes, curv


def backward_layer(back, tans, slopes, curv):
    inner = back[1] * tans[0]
    for grad, tan in zip(back[2:], tans[1:]):
        inner = inner + grad * tan
    pre = back[0] * slopes + curv * inner
    signal = stack([pre.astype(BF16)] + [(grad * slopes).astype(BF16) for grad in back[1:]])
    return pre, signal


def first_kernel(ids, packed, w_in, b_in, w_mid, send, keep, layer):
    step = pl.program_id(0)
    half = pl.num_programs(0) // 2
    rows = packed.shape[0]

    @pl.when(step == 0)
    def _():
        inputs = packed_rows(packed[...], w_in.shape[0])
        pieces = rows_of(mm(inputs, w_in[...], NN), rows)
        layer[...] = forward_layer(pieces, b_in[...].astype(F32))[0]

    part = mm(layer[...], w_mid[...], NN).astype(BF16)

    @pl.when(step < half)
    def _():
        send[0] = part

    @pl.when(step >= half)
    def _():
        keep[0] = part


def score_kernel(ids, packed, h_keep, h_recv, b_mid, w_out, b_out, loss, score_hl, parts):
    me = ids[0]
    rows, patch = packed.shape[0], w_out.shape[2]
    n_blocks = w_out.shape[0]
    inputs = packed_rows(packed[...], patch)
    for r in range(n_blocks):
        block = me ^ r
        h_ref = h_recv if r % 2 else h_keep
        pieces = rows_of(h_ref[r // 2].astype(F32), rows)
        layer = forward_layer(pieces, b_mid[block].astype(F32))[0]
        parts[block] = mm(layer, w_out[block], NN)
    total = parts[0]
    for b in range(1, n_blocks):
        total = total + parts[b]
    outs = rows_of(total, rows)
    dirs = rows_of(inputs.astype(F32), rows)[1:]
    score = outs[0] + b_out[...]
    grad = jnp.zeros_like(score)
    losses = jnp.zeros((rows, 1), F32)
    for vec, dscore in zip(dirs, outs[1:]):
        projected = jnp.sum(vec * score, axis=1, keepdims=True)
        traced = jnp.sum(vec * dscore, axis=1, keepdims=True)
        losses = losses + traced + 0.5 * projected * projected
        grad = grad + projected * vec
    loss[...] = losses / len(dirs)
    high = grad.astype(BF16)
    score_hl[...] = jnp.concatenate([high, (grad - high.astype(F32)).astype(BF16)], axis=1)


def back_kernel(ids, packed, score_hl, h_keep, h_recv, b_mid, w_out, w_mid, w_in, b_in, out):
    me = ids[0]
    rows, patch = packed.shape[0], w_out.shape[2]
    n_blocks, width = w_out.shape[0], w_out.shape[1]
    inputs = packed_rows(packed[...], patch)
    out_rows = stack([score_hl[:, :patch], inputs[rows:]])
    back_first = None
    for r in range(n_blocks):
        block = me ^ r
        h_ref = h_recv if r % 2 else h_keep
        pieces = rows_of(h_ref[r // 2].astype(F32), rows)
        _, slopes, curv = swish_terms(pieces[0] + b_mid[block].astype(F32))
        back = rows_of(mm(out_rows, w_out[block], NT), rows)
        signal = backward_layer(back, pieces[1:], slopes, curv)[1]
        cols = pl.ds(pl.multiple_of(block * width, width), width)
        term = mm(signal, w_mid[:, cols], NT)
        back_first = term if back_first is None else back_first + term
    pieces = rows_of(mm(inputs, w_in[...], NN), rows)
    _, slopes, curv = swish_terms(pieces[0] + b_in[...].astype(F32))
    pre, signal = backward_layer(rows_of(back_first, rows), pieces[1:], slopes, curv)
    out[:patch] = mm(inputs, signal, TN).astype(BF16)
    bias = jnp.sum(pre, axis=0, keepdims=True)
    out[patch:] = jnp.broadcast_to(bias, (out.shape[0] - patch, bias.shape[1])).astype(BF16)


def grads_kernel(ids, packed, score_hl, hid, b_mid, w_out, w_sel, b_sel, block_out, g_out, g_mid, g_bias, acc):
    step = pl.program_id(0)
    last = pl.num_programs(0) - 1
    rows, patch = packed.shape[1], w_out.shape[2]
    scale = 1.0 / (rows * pl.num_programs(0) * (packed.shape[2] // patch - 1))
    inputs = packed_rows(packed[0], patch)
    hl = score_hl[0]
    out_rows = stack([hl[:, :patch], inputs[rows:]])
    pieces = rows_of(hid[0].astype(F32), rows)
    layer_two, slopes, curv = forward_layer(pieces, b_mid[0].astype(F32))
    back = rows_of(mm(out_rows, w_out[0], NT), rows)
    pre, signal = backward_layer(back, pieces[1:], slopes, curv)
    layer_one = forward_layer(rows_of(mm(inputs, w_sel[...], NN), rows), b_sel[...].astype(F32))[0]
    mid = mm(layer_one, signal, TN)
    outg = mm(layer_two, out_rows, TN) * scale
    bias_mid = jnp.sum(pre, axis=0, keepdims=True) * scale
    both = jnp.sum(hl.astype(F32), axis=0, keepdims=True)
    bias_out = (both[:, :patch] + both[:, patch:]) * scale

    @pl.when(step == 0)
    def _():
        acc[...] = mid
        g_out[...] = outg
        g_mid[...] = bias_mid
        g_bias[...] = bias_out

    @pl.when(step > 0)
    def _():
        acc[...] += mid
        g_out[...] += outg
        g_mid[...] += bias_mid
        g_bias[...] += bias_out

    @pl.when(step == last)
    def _():
        width = block_out.shape[1]
        for r in range(block_out.shape[0]):
            block_out[r] = (acc[r * width : (r + 1) * width] * scale).astype(BF16)


def merge_kernel(ids, *refs):
    me = ids[0]
    out = refs[-1]
    width = refs[0].shape[1]
    for r, ref in enumerate(refs[:-1]):
        cols = pl.ds(pl.multiple_of((me ^ r) * width, width), width)
        out[:, cols] = ref[...].astype(F32)


def shape(dims, dtype):
    return jax.ShapeDtypeStruct(dims, dtype)


def whole(dims):
    return pl.BlockSpec(dims, lambda *_: (0,) * len(dims))


def call(body, grid, in_specs, out_specs, out_shape, scratch=()):
    return pl.pallas_call(
        body,
        grid_spec=pltpu.PrefetchScalarGridSpec(
            num_scalar_prefetch=1, grid=grid, in_specs=in_specs, out_specs=out_specs, scratch_shapes=list(scratch)
        ),
        out_shape=out_shape,
        name=body.__name__,
    )


def xor_move(x, axis, mask):
    return lax.ppermute(x, axis, [(i, i ^ mask) for i in range(lax.axis_size(axis))])


def pairwise(axis):
    size = lax.axis_size(axis)
    return size <= 8 and size & (size - 1) == 0


def doubling_gather(x, axis):
    if not pairwise(axis):
        return lax.all_gather(x, axis)
    out = x[None]
    mask = 1
    while mask < lax.axis_size(axis):
        out = jnp.concatenate([out, xor_move(out, axis, mask)], axis=0)
        mask *= 2
    return out


def bulk_gather(x, axis):
    if not pairwise(axis):
        return lax.all_gather(x, axis)
    size = lax.axis_size(axis)
    slots = {0: x}
    for mask in (2, 4, 6):
        if mask < size:
            slots[mask] = xor_move(x, axis, mask)
    for mask in list(slots):
        slots[mask ^ 1] = xor_move(slots[mask], axis, 1)
    return jnp.stack([slots[i] for i in range(size)], axis=0)


def pair_sum(x, axis):
    if not pairwise(axis):
        return lax.psum(x.astype(F32), axis)
    total = x.astype(F32)
    mask = 1
    while mask < lax.axis_size(axis):
        total = x.astype(F32) + xor_move(x, axis, mask).astype(F32)
        x = total.astype(BF16)
        mask *= 2
    return total


def shards(samples, projections, weight_in, bias_in, weight_mid, bias_mid, weight_out, bias_out):
    n_dp, n_t = lax.axis_size("dp"), lax.axis_size("tensor")
    d, t = lax.axis_index("dp"), lax.axis_index("tensor")
    rows, patch = samples.shape
    count = projections.shape[1] // patch
    full = rows * (count + 1)
    width = weight_in.shape[1]
    part = width // n_dp
    scale = 1.0 / (rows * n_dp * count)
    half = n_t // 2
    ids = jnp.stack([t, d]).astype(jnp.int32)
    packed = jnp.concatenate([samples, projections], axis=1)
    b_in = bias_in.reshape(1, width)
    b_mid = bias_mid.reshape(n_t, 1, width)
    w_out = weight_out.reshape(n_t, width, patch)
    b_out = bias_out.reshape(1, patch)

    send, keep = call(
        first_kernel,
        (n_t,),
        [
            whole(packed.shape),
            whole(weight_in.shape),
            whole(b_in.shape),
            pl.BlockSpec(
                (width, width),
                lambda i, ids: (0, ids[0] ^ jnp.where(i < half, 2 * i + 1, 2 * (i - half))),
            ),
        ],
        [
            pl.BlockSpec((1, full, width), lambda i, ids: (jnp.minimum(i, half - 1), 0, 0)),
            pl.BlockSpec((1, full, width), lambda i, ids: (jnp.maximum(i - half, 0), 0, 0)),
        ],
        [shape((half, full, width), BF16)] * 2,
        [pltpu.VMEM((full, width), BF16)],
    )(ids, packed, weight_in, b_in, weight_mid)

    got = xor_move(send, "tensor", 1)
    chip = (keep.astype(F32) + got.astype(F32)).astype(BF16)
    hidden = [chip[i].astype(F32) for i in range(half)]
    for q in range(1, half):
        for i in range(half):
            hidden[i] = hidden[i] + xor_move(chip[i ^ q], "tensor", 2 * q).astype(F32)
    own = hidden[0].astype(BF16)
    h_keep = jnp.stack([h.astype(BF16) for h in hidden], axis=0)
    h_recv = xor_move(h_keep, "tensor", 1)

    packed_all = doubling_gather(packed, "dp")
    sel = jnp.concatenate([weight_in, b_in, jnp.zeros((15, width), BF16)], axis=0)
    sel = doubling_gather(lax.dynamic_slice_in_dim(sel, d * part, part, 1), "tensor")
    sel = jnp.concatenate([sel[r] for r in range(n_t)], axis=1)
    w_sel, b_sel = sel[:patch], sel[patch : patch + 1]

    hid_all = bulk_gather(own, "dp")

    loss, score_hl = call(
        score_kernel,
        (1,),
        [whole(a.shape) for a in (packed, h_keep, h_recv, b_mid, w_out, b_out)],
        [whole((rows, 1)), whole((rows, 2 * patch))],
        [shape((rows, 1), F32), shape((rows, 2 * patch), BF16)],
        [pltpu.VMEM((n_t, full, patch), F32)],
    )(ids, packed, h_keep, h_recv, b_mid, w_out, b_out)
    score_all = doubling_gather(score_hl, "dp")

    in_rows = patch + 16
    summed = call(
        back_kernel,
        (1,),
        [
            whole(a.shape)
            for a in (packed, score_hl, h_keep, h_recv, b_mid, w_out, weight_mid, weight_in, b_in)
        ],
        whole((in_rows, width)),
        shape((in_rows, width), BF16),
    )(ids, packed, score_hl, h_keep, h_recv, b_mid, w_out, weight_mid, weight_in, b_in)

    mine = lambda i, ids: (i ^ ids[1] if pairwise("dp") else i, 0, 0)
    mid_block, g_out, g_mid, g_bias = call(
        grads_kernel,
        (n_dp,),
        [
            pl.BlockSpec((1,) + packed.shape, mine),
            pl.BlockSpec((1,) + score_hl.shape, mine),
            pl.BlockSpec((1, full, width), mine),
            pl.BlockSpec((1, 1, width), lambda i, ids: (ids[0], 0, 0)),
            pl.BlockSpec((1, width, patch), lambda i, ids: (ids[0], 0, 0)),
            whole(w_sel.shape),
            whole(b_sel.shape),
        ],
        [whole((n_t, part, width)), whole((width, patch)), whole((1, width)), whole((1, patch))],
        [shape((n_t, part, width), BF16), shape((width, patch), F32), shape((1, width), F32), shape((1, patch), F32)],
        [pltpu.VMEM((n_t * part, width), F32)],
    )(ids, packed_all, score_all, hid_all, b_mid, w_out, w_sel, b_sel)

    chunks = [mid_block[0]] + [xor_move(mid_block[r], "tensor", r) for r in range(1, n_t)]
    grad_mid = call(
        merge_kernel,
        (1,),
        [whole(c.shape) for c in chunks],
        whole((part, n_t * width)),
        shape((part, n_t * width), F32),
    )(ids, *chunks)

    total = pair_sum(summed, "dp") * scale
    return (
        loss.reshape(rows),
        total[:patch],
        total[patch],
        grad_mid,
        g_mid.reshape(width),
        g_out,
        g_bias.reshape(patch),
    )


def solution(mesh):
    placed = (
        P("dp", None),
        P("dp", None),
        P(None, "tensor"),
        P("tensor"),
        P("tensor", None),
        P(),
        P(),
        P(),
    )
    return jax.shard_map(
        shards,
        mesh=mesh,
        in_specs=placed,
        out_specs=(
            P("dp"),
            P(None, "tensor"),
            P("tensor"),
            P(("tensor", "dp"), None),
            P("tensor"),
            P("tensor", None),
            P(),
        ),
        check_vma=False,
    )
```

```python
import functools

import jax
import jax.numpy as jnp
from jax import lax
from jax.experimental import pallas as pl
from jax.experimental.pallas import tpu as pltpu
from jax.sharding import PartitionSpec as P


F32 = jnp.float32
BF16 = jnp.bfloat16
NN = (((1,), (0,)), ((), ()))
NT = (((1,), (1,)), ((), ()))
TN = (((0,), (0,)), ((), ()))


def mm(a, b, dims):
    return lax.dot_general(a, b, dims, preferred_element_type=F32)


def stack(parts):
    return jnp.concatenate(parts, axis=0)


def swish_terms(hidden):
    gate = jax.nn.sigmoid(hidden)
    slopes = gate * (1.0 + hidden * (1.0 - gate))
    curv = gate * (1.0 - gate) * (2.0 + hidden * (1.0 - 2.0 * gate))
    return hidden * gate, slopes, curv


def rows_of(full, rows):
    count = full.shape[0] // rows
    return [full[i * rows : (i + 1) * rows] for i in range(count)]


def vectors_of(projections, patch):
    count = projections.shape[1] // patch
    return [projections[:, i * patch : (i + 1) * patch] for i in range(count)]


def input_rows(samples, projections):
    return stack([samples] + vectors_of(projections, samples.shape[1]))


def row_vector(x):
    return x.astype(F32)[None, :]


def forward_layer(pieces, bias):
    act, slopes, curv = swish_terms(pieces[0] + bias)
    layer = stack([act.astype(BF16)] + [(slopes * tan).astype(BF16) for tan in pieces[1:]])
    return layer, slopes, curv


def backward_layer(back, tans, slopes, curv):
    inner = back[1] * tans[0]
    for grad, tan in zip(back[2:], tans[1:]):
        inner = inner + grad * tan
    pre = back[0] * slopes + curv * inner
    signal = stack([pre.astype(BF16)] + [(grad * slopes).astype(BF16) for grad in back[1:]])
    return pre, signal


def first_kernel(ids, samples, projections, w_in, b_in, w_mid, send, keep, w_buf, sems):
    me = ids[0]
    width = w_in.shape[1]
    n_blocks = w_buf.shape[0]
    order = [*range(1, n_blocks, 2), *range(0, n_blocks, 2)]
    copies = []
    for r in order:
        cols = pl.ds(pl.multiple_of((me ^ r) * width, width), width)
        copies.append(pltpu.make_async_copy(w_mid.at[:, cols], w_buf.at[r], sems.at[r]))
        copies[-1].start()
    inputs = input_rows(samples[...], projections[...])
    pieces = rows_of(mm(inputs, w_in[...], NN), samples.shape[0])
    layer = forward_layer(pieces, row_vector(b_in[...]))[0]
    for r, copy in zip(order, copies):
        copy.wait()
        out = send if r % 2 else keep
        out[r // 2] = mm(layer, w_buf[r], NN).astype(BF16)


def score_kernel(ids, projections, h_keep, h_recv, b_mid, w_out, b_out, loss, score_hl, parts):
    me = ids[0]
    patch, width = w_out.shape[0], h_keep.shape[2]
    n_blocks = w_out.shape[1] // width
    rows = projections.shape[0]
    for r in range(n_blocks):
        block = me ^ r
        cols = pl.ds(pl.multiple_of(block * width, width), width)
        h_ref = h_recv if r % 2 else h_keep
        pieces = rows_of(h_ref[r // 2].astype(F32), rows)
        layer = forward_layer(pieces, row_vector(b_mid[cols]))[0]
        parts[block] = mm(layer, w_out[:, cols], NT)
    total = parts[0]
    for b in range(1, n_blocks):
        total = total + parts[b]
    outs = rows_of(total, rows)
    dirs = [v.astype(F32) for v in vectors_of(projections[...], patch)]
    score = outs[0] + row_vector(b_out[...])
    grad = jnp.zeros_like(score)
    losses = jnp.zeros((rows, 1), F32)
    for vec, dscore in zip(dirs, outs[1:]):
        projected = jnp.sum(vec * score, axis=1, keepdims=True)
        traced = jnp.sum(vec * dscore, axis=1, keepdims=True)
        losses = losses + traced + 0.5 * projected * projected
        grad = grad + projected * vec
    diagonal = lax.broadcasted_iota(jnp.int32, (rows, rows), 0) == lax.broadcasted_iota(jnp.int32, (rows, rows), 1)
    loss[...] = jnp.sum(jnp.where(diagonal, losses, 0.0), axis=0, keepdims=True) / len(dirs)
    high = grad.astype(BF16)
    score_hl[...] = jnp.concatenate([high, (grad - high.astype(F32)).astype(BF16)], axis=1)


def back_kernel(ids, samples, projections, score_hl, h_keep, h_recv, b_mid, w_out, w_mid, w_in, b_in, out):
    me = ids[0]
    patch, width = w_in.shape
    n_blocks = w_out.shape[1] // width
    rows = samples.shape[0]
    inputs = input_rows(samples[...], projections[...])
    out_rows = stack([score_hl[:, :patch], inputs[rows:]])
    back_first = None
    for r in range(n_blocks):
        cols = pl.ds(pl.multiple_of((me ^ r) * width, width), width)
        h_ref = h_recv if r % 2 else h_keep
        pieces = rows_of(h_ref[r // 2].astype(F32), rows)
        _, slopes, curv = swish_terms(pieces[0] + row_vector(b_mid[cols]))
        back = rows_of(mm(out_rows, w_out[:, cols], NN), rows)
        signal = backward_layer(back, pieces[1:], slopes, curv)[1]
        term = mm(signal, w_mid[:, cols], NT)
        back_first = term if back_first is None else back_first + term
    pieces = rows_of(mm(inputs, w_in[...], NN), rows)
    _, slopes, curv = swish_terms(pieces[0] + row_vector(b_in[...]))
    pre, signal = backward_layer(rows_of(back_first, rows), pieces[1:], slopes, curv)
    out[:patch] = mm(inputs, signal, TN).astype(BF16)
    bias = jnp.sum(pre, axis=0, keepdims=True)
    out[patch:] = jnp.broadcast_to(bias, (out.shape[0] - patch, width)).astype(BF16)


def grads_kernel(ids, packed, score_hl, hid, b_mid, w_out, w_sel, block_out, g_out, g_mid, g_bias, acc, acc_mid, acc_bias):
    n_dp, rows, span = packed.shape
    patch, width = w_out.shape[0], hid.shape[2]
    n_blocks, part = block_out.shape[0], block_out.shape[1]
    scale = 1.0 / (rows * n_dp * (span // patch - 1))
    cols = pl.ds(pl.multiple_of(ids[0] * width, width), width)
    mask = ids[1] if pairwise_size(n_dp) else 0
    w_own = w_out[:, cols]
    b_own = row_vector(b_mid[cols])
    b_sel = w_sel[patch : patch + 1].astype(F32)
    acc[...] = jnp.zeros_like(acc)
    g_out[...] = jnp.zeros_like(g_out)
    acc_mid[...] = jnp.zeros_like(acc_mid)
    acc_bias[...] = jnp.zeros_like(acc_bias)

    def body(step, carry):
        slot = step ^ mask
        inputs = input_rows(packed[slot][:, :patch], packed[slot][:, patch:])
        hl = score_hl[slot]
        out_rows = stack([hl[:, :patch], inputs[rows:]])
        pieces = rows_of(hid[slot].astype(F32), rows)
        layer_two, slopes, curv = forward_layer(pieces, b_own)
        back = rows_of(mm(out_rows, w_own, NN), rows)
        pre, signal = backward_layer(back, pieces[1:], slopes, curv)
        layer_one = forward_layer(rows_of(mm(inputs, w_sel[:patch], NN), rows), b_sel)[0]
        acc[...] += mm(layer_one, signal, TN)
        g_out[...] += mm(out_rows, layer_two, TN)
        acc_mid[...] += pre
        acc_bias[...] += hl.astype(F32)
        return carry

    lax.fori_loop(0, n_dp, body, 0, unroll=n_dp <= 8)
    g_out[...] = g_out[...] * scale
    g_mid[...] = jnp.sum(acc_mid[...], axis=0, keepdims=True) * scale
    both = jnp.sum(acc_bias[...], axis=0, keepdims=True)
    g_bias[...] = (both[:, :patch] + both[:, patch:]) * scale
    for r in range(n_blocks):
        block_out[r] = (acc[r * part : (r + 1) * part] * scale).astype(BF16)


def merge_kernel(scale, ids, *refs):
    me = ids[0]
    *chunks, mine, other, out, g_in, g_bias = refs
    width = mine.shape[1]
    patch = g_in.shape[0]
    for r, ref in enumerate(chunks):
        cols = pl.ds(pl.multiple_of((me ^ r) * width, width), width)
        out[:, cols] = ref[...].astype(F32)
    total = (mine[...].astype(F32) + other[...].astype(F32)) * scale
    g_in[...] = total[:patch]
    g_bias[...] = total[patch : patch + 1]


def shape(dims, dtype):
    return jax.ShapeDtypeStruct(dims, dtype)


def call(body, out_shape, args, scratch=(), raw=()):
    spaces = [pltpu.SMEM] + [pl.ANY if i in raw else pltpu.VMEM for i in range(1, len(args))]
    n_out = len(out_shape)
    return pl.pallas_call(
        body,
        in_specs=[pl.BlockSpec(memory_space=m) for m in spaces],
        out_specs=[pl.BlockSpec(memory_space=pltpu.VMEM)] * n_out,
        out_shape=out_shape,
        scratch_shapes=list(scratch),
        name=getattr(body, "__name__", "merge_kernel"),
    )(*args)


def xor_move(x, axis, mask):
    return lax.ppermute(x, axis, [(i, i ^ mask) for i in range(lax.axis_size(axis))])


def pairwise_size(size):
    return size <= 8 and size & (size - 1) == 0


def pairwise(axis):
    return pairwise_size(lax.axis_size(axis))


def doubling_gather(x, axis):
    if not pairwise(axis):
        return lax.all_gather(x, axis)
    out = x[None]
    mask = 1
    while mask < lax.axis_size(axis):
        out = jnp.concatenate([out, xor_move(out, axis, mask)], axis=0)
        mask *= 2
    return out


def bulk_gather(x, axis):
    if not pairwise(axis):
        return lax.all_gather(x, axis)
    size = lax.axis_size(axis)
    slots = {0: x}
    for mask in (2, 4, 6):
        if mask < size:
            slots[mask] = xor_move(x, axis, mask)
    for mask in list(slots):
        slots[mask ^ 1] = xor_move(slots[mask], axis, 1)
    return jnp.stack([slots[i] for i in range(size)], axis=0)


def pair_sum(x, axis):
    if not pairwise(axis):
        return lax.psum(x.astype(F32), axis), jnp.zeros_like(x)
    mask = 1
    while 2 * mask < lax.axis_size(axis):
        x = (x.astype(F32) + xor_move(x, axis, mask).astype(F32)).astype(BF16)
        mask *= 2
    return x, xor_move(x, axis, mask)


def shards(samples, projections, weight_in, bias_in, weight_mid, bias_mid, weight_out, bias_out):
    n_dp, n_t = lax.axis_size("dp"), lax.axis_size("tensor")
    d, t = lax.axis_index("dp"), lax.axis_index("tensor")
    rows, patch = samples.shape
    count = projections.shape[1] // patch
    full = rows * (count + 1)
    width = weight_in.shape[1]
    part = width // n_dp
    scale = 1.0 / (rows * n_dp * count)
    half = n_t // 2
    ids = jnp.stack([t, d]).astype(jnp.int32)
    w_out = weight_out.T

    send, keep = call(
        first_kernel,
        [shape((half, full, width), BF16)] * 2,
        (ids, samples, projections, weight_in, bias_in, weight_mid),
        [pltpu.VMEM((n_t, width, width), BF16), pltpu.SemaphoreType.DMA((n_t,))],
        raw=(5,),
    )

    got = xor_move(send, "tensor", 1)
    chip = [(keep[i].astype(F32) + got[i].astype(F32)).astype(BF16) for i in range(half)]
    hidden = [c.astype(F32) for c in chip]
    for q in range(1, half):
        for i in range(half):
            hidden[i] = hidden[i] + xor_move(chip[i ^ q], "tensor", 2 * q).astype(F32)
    own = hidden[0].astype(BF16)
    h_keep = jnp.stack([h.astype(BF16) for h in hidden], axis=0)
    h_recv = xor_move(h_keep, "tensor", 1)

    packed = jnp.concatenate([samples, projections], axis=1)
    packed_all = doubling_gather(packed, "dp")
    sel = jnp.concatenate([weight_in, bias_in[None, :], jnp.zeros((15, width), BF16)], axis=0)
    sel = doubling_gather(lax.dynamic_slice_in_dim(sel, d * part, part, 1), "tensor")
    w_sel = jnp.concatenate([sel[r] for r in range(n_t)], axis=1)

    hid_all = bulk_gather(own, "dp")

    loss, score_hl = call(
        score_kernel,
        [shape((1, rows), F32), shape((rows, 2 * patch), BF16)],
        (ids, projections, h_keep, h_recv, bias_mid, w_out, bias_out),
        [pltpu.VMEM((n_t, full, patch), F32)],
    )
    score_all = doubling_gather(score_hl, "dp")

    (summed,) = call(
        back_kernel,
        [shape((patch + 16, width), BF16)],
        (ids, samples, projections, score_hl, h_keep, h_recv, bias_mid, w_out, weight_mid, weight_in, bias_in),
    )

    mid_block, g_out, g_mid, g_bias = call(
        grads_kernel,
        [shape((n_t, part, width), BF16), shape((patch, width), F32), shape((1, width), F32), shape((1, patch), F32)],
        (ids, packed_all, score_all, hid_all, bias_mid, w_out, w_sel),
        [pltpu.VMEM((n_t * part, width), F32), pltpu.VMEM((rows, width), F32), pltpu.VMEM((rows, 2 * patch), F32)],
    )

    chunks = [mid_block[0]] + [xor_move(mid_block[r], "tensor", r) for r in range(1, n_t)]
    grad_mid, g_in, g_bias_in = call(
        functools.partial(merge_kernel, scale),
        [shape((part, n_t * width), F32), shape((patch, width), F32), shape((1, width), F32)],
        (ids, *chunks, *pair_sum(summed, "dp")),
    )
    return (
        loss.reshape(rows),
        g_in,
        g_bias_in.reshape(width),
        grad_mid,
        g_mid.reshape(width),
        g_out.T,
        g_bias.reshape(patch),
    )


def solution(mesh):
    placed = (
        P("dp", None),
        P("dp", None),
        P(None, "tensor"),
        P("tensor"),
        P("tensor", None),
        P(),
        P(),
        P(),
    )
    return jax.shard_map(
        shards,
        mesh=mesh,
        in_specs=placed,
        out_specs=(
            P("dp"),
            P(None, "tensor"),
            P("tensor"),
            P(("tensor", "dp"), None),
            P("tensor"),
            P("tensor", None),
            P(),
        ),
        check_vma=False,
    )
```

```python
import functools

import jax
import jax.numpy as jnp
from jax import lax
from jax.experimental import pallas as pl
from jax.experimental.pallas import tpu as pltpu
from jax.sharding import PartitionSpec as P


VMEM_BYTES = 16 * 2**20
F32 = jnp.float32
BF16 = jnp.bfloat16
NN = (((1,), (0,)), ((), ()))
NT = (((1,), (1,)), ((), ()))
TN = (((0,), (0,)), ((), ()))


def mm(a, b, dims):
    return lax.dot_general(a, b, dims, preferred_element_type=F32)


def stack(parts):
    return jnp.concatenate(parts, axis=0)


def swish_terms(hidden):
    gate = jax.nn.sigmoid(hidden)
    slopes = gate * (1.0 + hidden * (1.0 - gate))
    curv = gate * (1.0 - gate) * (2.0 + hidden * (1.0 - 2.0 * gate))
    return hidden * gate, slopes, curv


def rows_of(full, rows):
    count = full.shape[0] // rows
    return [full[i * rows : (i + 1) * rows] for i in range(count)]


def vectors_of(projections, patch):
    count = projections.shape[1] // patch
    return [projections[:, i * patch : (i + 1) * patch] for i in range(count)]


def input_rows(samples, projections):
    return stack([samples] + vectors_of(projections, samples.shape[1]))


def row_vector(x):
    return x.astype(F32)[None, :]


def forward_layer(pieces, bias):
    act, slopes, curv = swish_terms(pieces[0] + bias)
    layer = stack([act.astype(BF16)] + [(slopes * tan).astype(BF16) for tan in pieces[1:]])
    return layer, slopes, curv


def backward_layer(back, tans, slopes, curv):
    inner = back[1] * tans[0]
    for grad, tan in zip(back[2:], tans[1:]):
        inner = inner + grad * tan
    pre = back[0] * slopes + curv * inner
    signal = stack([pre.astype(BF16)] + [(grad * slopes).astype(BF16) for grad in back[1:]])
    return pre, signal


def first_kernel(ids, samples, projections, w_in, b_in, w_mid, send, keep, w_buf, sems):
    me = ids[0]
    width = w_in.shape[1]
    n_blocks = w_buf.shape[0]
    order = [*range(1, n_blocks, 2), *range(0, n_blocks, 2)]
    copies = []
    for r in order:
        cols = pl.ds(pl.multiple_of((me ^ r) * width, width), width)
        copies.append(pltpu.make_async_copy(w_mid.at[:, cols], w_buf.at[r], sems.at[r]))
        copies[-1].start()
    inputs = input_rows(samples[...], projections[...])
    pieces = rows_of(mm(inputs, w_in[...], NN), samples.shape[0])
    layer = forward_layer(pieces, row_vector(b_in[...]))[0]
    for r, copy in zip(order, copies):
        copy.wait()
        out = send if r % 2 else keep
        out[r // 2] = mm(layer, w_buf[r], NN).astype(BF16)


def score_kernel(ids, samples, projections, h_keep, h_recv, b_mid, w_out, b_out, loss, info, parts):
    me = ids[0]
    patch, width = w_out.shape[0], h_keep.shape[2]
    n_blocks = w_out.shape[1] // width
    rows = projections.shape[0]
    for r in range(n_blocks):
        block = me ^ r
        cols = pl.ds(pl.multiple_of(block * width, width), width)
        h_ref = h_recv if r % 2 else h_keep
        pieces = rows_of(h_ref[r // 2].astype(F32), rows)
        layer = forward_layer(pieces, row_vector(b_mid[cols]))[0]
        parts[block] = mm(layer, w_out[:, cols], NT)
    total = parts[0]
    for b in range(1, n_blocks):
        total = total + parts[b]
    outs = rows_of(total, rows)
    dirs = [v.astype(F32) for v in vectors_of(projections[...], patch)]
    score = outs[0] + row_vector(b_out[...])
    grad = jnp.zeros_like(score)
    losses = jnp.zeros((rows, 1), F32)
    for vec, dscore in zip(dirs, outs[1:]):
        projected = jnp.sum(vec * score, axis=1, keepdims=True)
        traced = jnp.sum(vec * dscore, axis=1, keepdims=True)
        losses = losses + traced + 0.5 * projected * projected
        grad = grad + projected * vec
    diagonal = lax.broadcasted_iota(jnp.int32, (rows, rows), 0) == lax.broadcasted_iota(jnp.int32, (rows, rows), 1)
    loss[...] = jnp.sum(jnp.where(diagonal, losses, 0.0), axis=0, keepdims=True) / len(dirs)
    high = grad.astype(BF16)
    low = (grad - high.astype(F32)).astype(BF16)
    info[...] = jnp.concatenate([high, low, samples[...], projections[...]], axis=1)


def back_kernel(ids, samples, projections, info, h_keep, h_recv, b_mid, w_out, w_mid, w_in, b_in, out):
    me = ids[0]
    patch, width = w_in.shape
    n_blocks = w_out.shape[1] // width
    rows = samples.shape[0]
    inputs = input_rows(samples[...], projections[...])
    out_rows = stack([info[:, :patch], inputs[rows:]])
    back_first = None
    for r in range(n_blocks):
        cols = pl.ds(pl.multiple_of((me ^ r) * width, width), width)
        h_ref = h_recv if r % 2 else h_keep
        pieces = rows_of(h_ref[r // 2].astype(F32), rows)
        _, slopes, curv = swish_terms(pieces[0] + row_vector(b_mid[cols]))
        back = rows_of(mm(out_rows, w_out[:, cols], NN), rows)
        signal = backward_layer(back, pieces[1:], slopes, curv)[1]
        term = mm(signal, w_mid[:, cols], NT)
        back_first = term if back_first is None else back_first + term
    pieces = rows_of(mm(inputs, w_in[...], NN), rows)
    _, slopes, curv = swish_terms(pieces[0] + row_vector(b_in[...]))
    pre, signal = backward_layer(rows_of(back_first, rows), pieces[1:], slopes, curv)
    out[:patch] = mm(inputs, signal, TN).astype(BF16)
    bias = jnp.sum(pre, axis=0, keepdims=True)
    out[patch:] = jnp.broadcast_to(bias, (out.shape[0] - patch, width)).astype(BF16)


def grads_kernel(ids, info, hid, b_mid, w_out, w_sel, block_out, g_out, g_mid, g_bias, acc, acc_mid, acc_bias):
    n_dp, rows, span = info.shape
    patch, width = w_out.shape[0], hid.shape[2]
    n_blocks, part = block_out.shape[0], block_out.shape[1]
    scale = 1.0 / (rows * n_dp * (span // patch - 3))
    cols = pl.ds(pl.multiple_of(ids[0] * width, width), width)
    mask = ids[1] if pairwise_size(n_dp) else 0
    w_own = w_out[:, cols]
    b_own = row_vector(b_mid[cols])
    b_sel = w_sel[patch : patch + 1].astype(F32)
    acc[...] = jnp.zeros_like(acc)
    g_out[...] = jnp.zeros_like(g_out)
    acc_mid[...] = jnp.zeros_like(acc_mid)
    acc_bias[...] = jnp.zeros_like(acc_bias)

    def body(step, carry):
        slot = step ^ mask
        known = info[slot]
        hl = known[:, : 2 * patch]
        inputs = stack(vectors_of(known, patch)[2:])
        out_rows = stack([hl[:, :patch], inputs[rows:]])
        pieces = rows_of(hid[slot].astype(F32), rows)
        layer_two, slopes, curv = forward_layer(pieces, b_own)
        back = rows_of(mm(out_rows, w_own, NN), rows)
        pre, signal = backward_layer(back, pieces[1:], slopes, curv)
        layer_one = forward_layer(rows_of(mm(inputs, w_sel[:patch], NN), rows), b_sel)[0]
        acc[...] += mm(layer_one, signal, TN)
        g_out[...] += mm(out_rows, layer_two, TN)
        acc_mid[...] += pre
        acc_bias[...] += hl.astype(F32)
        return carry

    lax.fori_loop(0, n_dp, body, 0, unroll=n_dp <= 8)
    g_out[...] = g_out[...] * scale
    g_mid[...] = jnp.sum(acc_mid[...], axis=0, keepdims=True) * scale
    both = jnp.sum(acc_bias[...], axis=0, keepdims=True)
    g_bias[...] = (both[:, :patch] + both[:, patch:]) * scale
    for r in range(n_blocks):
        block_out[r] = (acc[r * part : (r + 1) * part] * scale).astype(BF16)


def merge_kernel(scale, ids, *refs):
    me = ids[0]
    *chunks, mine, other, out, g_in, g_bias = refs
    width = mine.shape[1]
    patch = g_in.shape[0]
    for r, ref in enumerate(chunks):
        cols = pl.ds(pl.multiple_of((me ^ r) * width, width), width)
        out[:, cols] = ref[...].astype(F32)
    total = (mine[...].astype(F32) + other[...].astype(F32)) * scale
    g_in[...] = total[:patch]
    g_bias[...] = total[patch : patch + 1]


def shape(dims, dtype):
    return jax.ShapeDtypeStruct(dims, dtype)


def near_shape(dims, dtype):
    return pltpu.VMEM(dims, dtype)


def call(body, out_shape, args, scratch=(), raw=(), near=(), far=()):
    spaces = [pltpu.SMEM] + [pl.ANY if i in raw else pltpu.VMEM for i in range(1, len(args))]
    args = [pltpu.with_memory_space_constraint(a, pltpu.VMEM) if i in near else a for i, a in enumerate(args)]
    args = [pltpu.with_memory_space_constraint(a, pltpu.HBM) if i in far else a for i, a in enumerate(args)]
    return pl.pallas_call(
        body,
        in_specs=[pl.BlockSpec(memory_space=m) for m in spaces],
        out_specs=[pl.BlockSpec(memory_space=pltpu.VMEM)] * len(out_shape),
        out_shape=out_shape,
        scratch_shapes=list(scratch),
        compiler_params=pltpu.CompilerParams(vmem_limit_bytes=VMEM_BYTES),
    )(*args)


def xor_move(x, axis, mask):
    return lax.ppermute(x, axis, [(i, i ^ mask) for i in range(lax.axis_size(axis))])


def pairwise_size(size):
    return size <= 8 and size & (size - 1) == 0


def pairwise(axis):
    return pairwise_size(lax.axis_size(axis))


def doubling_gather(x, axis):
    if not pairwise(axis):
        return lax.all_gather(x, axis)
    out = x[None]
    mask = 1
    while mask < lax.axis_size(axis):
        out = jnp.concatenate([out, xor_move(out, axis, mask)], axis=0)
        mask *= 2
    return out


def bulk_gather(x, axis):
    if not pairwise(axis):
        return lax.all_gather(x, axis)
    size = lax.axis_size(axis)
    slots = {0: x}
    for mask in (2, 4, 6):
        if mask < size:
            slots[mask] = xor_move(x, axis, mask)
    for mask in list(slots):
        slots[mask ^ 1] = xor_move(slots[mask], axis, 1)
    return jnp.stack([slots[i] for i in range(size)], axis=0)


def pair_sum(x, axis):
    if not pairwise(axis):
        return lax.psum(x.astype(F32), axis), jnp.zeros_like(x)
    mask = 1
    while 2 * mask < lax.axis_size(axis):
        x = (x.astype(F32) + xor_move(x, axis, mask).astype(F32)).astype(BF16)
        mask *= 2
    return x, xor_move(x, axis, mask)


def shards(samples, projections, weight_in, bias_in, weight_mid, bias_mid, weight_out, bias_out):
    n_dp, n_t = lax.axis_size("dp"), lax.axis_size("tensor")
    d, t = lax.axis_index("dp"), lax.axis_index("tensor")
    rows, patch = samples.shape
    count = projections.shape[1] // patch
    full = rows * (count + 1)
    width = weight_in.shape[1]
    part = width // n_dp
    scale = 1.0 / (rows * n_dp * count)
    half = n_t // 2
    ids = jnp.stack([t, d]).astype(jnp.int32)
    w_out = weight_out.T

    send, keep = call(
        first_kernel,
        [near_shape((half, full, width), BF16)] * 2,
        (ids, samples, projections, weight_in, bias_in, weight_mid),
        [pltpu.VMEM((n_t, width, width), BF16), pltpu.SemaphoreType.DMA((n_t,))],
        raw=(5,),
        far=(1, 2, 3, 4, 5),
    )

    got = xor_move(send, "tensor", 1)
    chip = [(keep[i].astype(F32) + got[i].astype(F32)).astype(BF16) for i in range(half)]
    chip = lax.optimization_barrier(chip)
    hidden = [c.astype(F32) for c in chip]
    for q in range(1, half):
        for i in range(half):
            hidden[i] = hidden[i] + xor_move(chip[i ^ q], "tensor", 2 * q).astype(F32)
    own = hidden[0].astype(BF16)
    h_keep = jnp.stack([h.astype(BF16) for h in hidden], axis=0)
    h_recv = xor_move(h_keep, "tensor", 1)

    sel = jnp.concatenate([weight_in, bias_in[None, :], jnp.zeros((15, width), BF16)], axis=0)
    sel = doubling_gather(lax.dynamic_slice_in_dim(sel, d * part, part, 1), "tensor")
    w_sel = jnp.concatenate([sel[r] for r in range(n_t)], axis=1)

    hid_all = bulk_gather(own, "dp")

    loss, info = call(
        score_kernel,
        [shape((1, rows), F32), near_shape((rows, (3 + count) * patch), BF16)],
        (ids, samples, projections, h_keep, h_recv, bias_mid, w_out, bias_out),
        [pltpu.VMEM((n_t, full, patch), F32)],
        near=(3, 4, 6),
    )
    info_all = doubling_gather(info, "dp")

    (summed,) = call(
        back_kernel,
        [near_shape((patch + 16, width), BF16)],
        (ids, samples, projections, info, h_keep, h_recv, bias_mid, w_out, weight_mid, weight_in, bias_in),
        near=(3, 4, 5, 7, 8),
    )

    mid_block, g_out, g_mid, g_bias = call(
        grads_kernel,
        [near_shape((n_t, part, width), BF16), shape((patch, width), F32), shape((1, width), F32), shape((1, patch), F32)],
        (ids, info_all, hid_all, bias_mid, w_out, w_sel),
        [pltpu.VMEM((n_t * part, width), F32), pltpu.VMEM((rows, width), F32), pltpu.VMEM((rows, 2 * patch), F32)],
        near=(1, 2, 4, 5) if pairwise("dp") else (),
    )

    chunks = [mid_block[0]] + [xor_move(mid_block[r], "tensor", r) for r in range(1, n_t)]
    grad_mid, g_in, g_bias_in = call(
        functools.partial(merge_kernel, scale),
        [shape((part, n_t * width), F32), shape((patch, width), F32), shape((1, width), F32)],
        (ids, *chunks, *pair_sum(summed, "dp")),
        near=tuple(range(1, n_t + 3)),
    )
    return (
        loss.reshape(rows),
        g_in,
        g_bias_in.reshape(width),
        grad_mid,
        g_mid.reshape(width),
        g_out.T,
        g_bias.reshape(patch),
    )


def solution(mesh):
    placed = (
        P("dp", None),
        P("dp", None),
        P(None, "tensor"),
        P("tensor"),
        P("tensor", None),
        P(),
        P(),
        P(),
    )

    return jax.shard_map(
        shards,
        mesh=mesh,
        in_specs=placed,
        out_specs=(
            P("dp"),
            P(None, "tensor"),
            P("tensor"),
            P(("tensor", "dp"), None),
            P("tensor"),
            P("tensor", None),
            P(),
        ),
        check_vma=False,
    )
```

```python
import functools

import jax
import jax.numpy as jnp
from jax import lax
from jax.experimental import pallas as pl
from jax.experimental.pallas import tpu as pltpu
from jax.sharding import PartitionSpec as P


VMEM_BYTES = 16 * 2**20
F32 = jnp.float32
BF16 = jnp.bfloat16
NN = (((1,), (0,)), ((), ()))
NT = (((1,), (1,)), ((), ()))
TN = (((0,), (0,)), ((), ()))


def mm(a, b, dims):
    return lax.dot_general(a, b, dims, preferred_element_type=F32)


def stack(parts):
    return jnp.concatenate(parts, axis=0)


def swish_terms(hidden):
    gate = jax.nn.sigmoid(hidden)
    slopes = gate * (1.0 + hidden * (1.0 - gate))
    curv = gate * (1.0 - gate) * (2.0 + hidden * (1.0 - 2.0 * gate))
    return hidden * gate, slopes, curv


def rows_of(full, rows):
    count = full.shape[0] // rows
    return [full[i * rows : (i + 1) * rows] for i in range(count)]


def vectors_of(projections, patch):
    count = projections.shape[1] // patch
    return [projections[:, i * patch : (i + 1) * patch] for i in range(count)]


def input_rows(samples, projections):
    return stack([samples] + vectors_of(projections, samples.shape[1]))


def row_vector(x):
    return x.astype(F32)[None, :]


def forward_layer(pieces, bias):
    act, slopes, curv = swish_terms(pieces[0] + bias)
    layer = stack([act.astype(BF16)] + [(slopes * tan).astype(BF16) for tan in pieces[1:]])
    return layer, slopes, curv


def backward_layer(back, tans, slopes, curv):
    inner = back[1] * tans[0]
    for grad, tan in zip(back[2:], tans[1:]):
        inner = inner + grad * tan
    pre = back[0] * slopes + curv * inner
    signal = stack([pre.astype(BF16)] + [(grad * slopes).astype(BF16) for grad in back[1:]])
    return pre, signal


def pack_weights(w_in, b_in, index, n_dp):
    patch, width = w_in.shape
    part, short = width // n_dp, patch // n_dp
    row = lax.broadcasted_iota(jnp.int32, (width, part), 0)
    col = lax.broadcasted_iota(jnp.int32, (width, part), 1)
    pick = jnp.where(row == col + index * part, 1.0, 0.0).astype(BF16)
    chosen = mm(w_in, pick, NN)
    bias = mm(jnp.broadcast_to(b_in, (short, width)).astype(BF16), pick, NN)
    wide = jnp.concatenate(rows_of(chosen, short), axis=1)
    rest = jnp.concatenate([bias, jnp.zeros((short, width - part), F32)], axis=1)
    return stack([wide, rest]).astype(BF16)


def unpack_weights(packs, n_dp):
    weights, biases = [], []
    for pack in packs:
        short = pack.shape[0] // 2
        part = pack.shape[1] // n_dp
        weights.append(stack(vectors_of(pack[:short], part)))
        biases.append(pack[short : short + 1, :part])
    return jnp.concatenate(weights, axis=1).astype(BF16), jnp.concatenate(biases, axis=1)


def pack_inputs(inputs, out_rows, width):
    short = 8
    pieces = rows_of(inputs.astype(F32), short)
    wide = width // inputs.shape[1]
    pieces += [jnp.zeros_like(pieces[0])] * (out_rows // short * wide - len(pieces))
    groups = [jnp.concatenate(pieces[i : i + wide], axis=1) for i in range(0, len(pieces), wide)]
    return stack(groups).astype(BF16)


def unpack_inputs(packed, full, patch):
    short = 8
    pieces = [v for group in rows_of(packed.astype(F32), short) for v in vectors_of(group, patch)]
    return stack(pieces[: full // short]).astype(BF16)


def first_kernel(n_dp, ids, samples, projections, w_in, b_in, w_mid, send, keep, known, w_buf, sems):
    me = ids[0]
    width = w_in.shape[1]
    n_blocks = w_buf.shape[0]
    full = samples.shape[0] * (1 + projections.shape[1] // samples.shape[1])
    order = [*range(1, n_blocks, 2), *range(0, n_blocks, 2)]
    copies = []
    for r in order:
        cols = pl.ds(pl.multiple_of((me ^ r) * width, width), width)
        copies.append(pltpu.make_async_copy(w_mid.at[:, cols], w_buf.at[r], sems.at[r]))
        copies[-1].start()
    inputs = input_rows(samples[...], projections[...])
    pieces = rows_of(mm(inputs, w_in[...], NN), samples.shape[0])
    layer = forward_layer(pieces, row_vector(b_in[...]))[0]
    known[...] = pack_inputs(inputs, known.shape[0], width)
    base = n_blocks // 2 * full
    if send.shape[0] > base:
        packed = pack_weights(w_in[...], row_vector(b_in[...]), ids[1], n_dp)
        send[base:] = packed
        keep[base:] = packed
    for r, copy in zip(order, copies):
        copy.wait()
        out = send if r % 2 else keep
        out[r // 2 * full : (r // 2 + 1) * full] = mm(layer, w_buf[r], NN).astype(BF16)


def score_kernel(ids, projections, h_keep, h_recv, b_mid, w_out, b_out, loss, info, parts):
    me = ids[0]
    patch, width = w_out.shape[0], h_keep.shape[2]
    n_blocks = w_out.shape[1] // width
    rows = projections.shape[0]
    for r in range(n_blocks):
        block = me ^ r
        cols = pl.ds(pl.multiple_of(block * width, width), width)
        h_ref = h_recv if r % 2 else h_keep
        pieces = rows_of(h_ref[r // 2].astype(F32), rows)
        layer = forward_layer(pieces, row_vector(b_mid[cols]))[0]
        parts[block] = mm(layer, w_out[:, cols], NT)
    total = parts[0]
    for b in range(1, n_blocks):
        total = total + parts[b]
    outs = rows_of(total, rows)
    dirs = [v.astype(F32) for v in vectors_of(projections[...], patch)]
    score = outs[0] + row_vector(b_out[...])
    grad = jnp.zeros_like(score)
    losses = jnp.zeros((rows, 1), F32)
    for vec, dscore in zip(dirs, outs[1:]):
        projected = jnp.sum(vec * score, axis=1, keepdims=True)
        traced = jnp.sum(vec * dscore, axis=1, keepdims=True)
        losses = losses + traced + 0.5 * projected * projected
        grad = grad + projected * vec
    diagonal = lax.broadcasted_iota(jnp.int32, (rows, rows), 0) == lax.broadcasted_iota(jnp.int32, (rows, rows), 1)
    loss[...] = jnp.sum(jnp.where(diagonal, losses, 0.0), axis=0, keepdims=True) / len(dirs)
    high = grad.astype(BF16)
    low = (grad - high.astype(F32)).astype(BF16)
    info[...] = jnp.concatenate([high, low], axis=1)


def back_kernel(ids, samples, projections, info, h_keep, h_recv, b_mid, w_out, w_mid, w_in, b_in, out):
    me = ids[0]
    patch, width = w_in.shape
    n_blocks = w_out.shape[1] // width
    rows = samples.shape[0]
    inputs = input_rows(samples[...], projections[...])
    out_rows = stack([info[:, :patch], inputs[rows:]])
    back_first = None
    for r in range(n_blocks):
        cols = pl.ds(pl.multiple_of((me ^ r) * width, width), width)
        h_ref = h_recv if r % 2 else h_keep
        pieces = rows_of(h_ref[r // 2].astype(F32), rows)
        _, slopes, curv = swish_terms(pieces[0] + row_vector(b_mid[cols]))
        back = rows_of(mm(out_rows, w_out[:, cols], NN), rows)
        signal = backward_layer(back, pieces[1:], slopes, curv)[1]
        term = mm(signal, w_mid[:, cols], NT)
        back_first = term if back_first is None else back_first + term
    pieces = rows_of(mm(inputs, w_in[...], NN), rows)
    _, slopes, curv = swish_terms(pieces[0] + row_vector(b_in[...]))
    pre, signal = backward_layer(rows_of(back_first, rows), pieces[1:], slopes, curv)
    out[:patch] = mm(inputs, signal, TN).astype(BF16)
    bias = jnp.sum(pre, axis=0, keepdims=True)
    high = info[:, :patch].astype(F32)
    score = jnp.sum(high + info[:, patch:].astype(F32), axis=0, keepdims=True)
    score = jnp.concatenate([score, jnp.zeros((1, width - patch), F32)], axis=1)
    short = (out.shape[0] - patch) // 2
    wide = jnp.concatenate(rows_of(high, short), axis=1)
    wide = jnp.concatenate([wide, jnp.zeros((short, width - wide.shape[1]), F32)], axis=1)
    out[patch:] = stack([bias, score, jnp.zeros((short - 2, width), F32), wide]).astype(BF16)


def grads_kernel(scale, n_dp, rows, full, n_before, final, ids, scores, hid, b_mid, w_out, w_near, w_far, *refs):
    count = hid.shape[0]
    before, refs = refs[: 2 * n_before + min(n_before, 1)], refs[2 * n_before + min(n_before, 1) :]
    acc, acc_out, acc_mid = refs[-3:]
    patch, width = w_out.shape[0], hid.shape[2]
    cols = pl.ds(pl.multiple_of(ids[0] * width, width), width)
    w_own = w_out[:, cols]
    b_own = row_vector(b_mid[cols])
    paired = w_near.shape[1] == width
    if paired:
        pairs = w_near[...].astype(F32), w_far[...].astype(F32)
        w_sel, b_sel = unpack_weights([p for pair in pairs for p in rows_of(pair, pair.shape[0] // 2)], n_dp)
    else:
        w_sel, b_sel = w_near[:patch], w_near[patch : patch + 1].astype(F32)

    def terms(slot):
        inputs = unpack_inputs(hid[slot, full:], full, patch)
        groups = rows // scores.shape[1]
        score = stack(vectors_of(scores[slot].astype(F32), patch)[:groups]).astype(BF16)
        out_rows = stack([score, inputs[rows:]])
        pieces = rows_of(hid[slot, :full].astype(F32), rows)
        layer_two, slopes, curv = forward_layer(pieces, b_own)
        back = rows_of(mm(out_rows, w_own, NN), rows)
        pre, signal = backward_layer(back, pieces[1:], slopes, curv)
        layer_one = forward_layer(rows_of(mm(inputs, w_sel, NN), rows), b_sel)[0]
        return mm(layer_one, signal, TN), mm(out_rows, layer_two, TN), pre

    if paired:
        mask = ids[1] & (count - 1)
        total = before[0][...] if n_before else None
        folded = None
        for step in range(0, count, 2):
            one, two = terms(step ^ mask), terms((step + 1) ^ mask)
            total = one[0] + two[0] if total is None else total + one[0] + two[0]
            pair = one[1] + two[1], one[2] + two[2]
            folded = pair if folded is None else (folded[0] + pair[0], folded[1] + pair[1])
        acc[...] = total
        acc_out[...], acc_mid[...] = folded
    else:
        for ref in (acc, acc_out, acc_mid):
            ref[...] = jnp.zeros_like(ref)

        def body(step, carry):
            for ref, term in zip((acc, acc_out, acc_mid), terms(step)):
                ref[...] += term
            return carry

        lax.fori_loop(0, count, body, 0)
        if n_before:
            acc[...] += before[0][...]
    if not final:
        return
    block_out, g_out, g_mid = refs[:3]
    n_blocks, part = block_out.shape[0], block_out.shape[1]
    out, mid = acc_out[...], acc_mid[...]
    for i in reversed(range(n_before)):
        out = out + before[1 + 2 * i][...]
        mid = mid + before[2 + 2 * i][...]
    g_out[...] = out * scale
    g_mid[...] = jnp.sum(mid, axis=0, keepdims=True) * scale
    for r in range(n_blocks):
        block_out[r] = (acc[r * part : (r + 1) * part] * scale).astype(BF16)


def merge_kernel(scale, ids, *refs):
    me = ids[0]
    *chunks, mine, other, out, g_in, g_bias, g_last = refs
    width = mine.shape[1]
    patch = g_in.shape[0]
    for r, ref in enumerate(chunks):
        cols = pl.ds(pl.multiple_of((me ^ r) * width, width), width)
        out[:, cols] = ref[...].astype(F32)
    total = (mine[...].astype(F32) + other[...].astype(F32)) * scale
    g_in[...] = total[:patch]
    g_bias[...] = total[patch : patch + 1]
    g_last[...] = total[patch + 1 : patch + 2, :patch]


def shape(dims, dtype):
    return jax.ShapeDtypeStruct(dims, dtype)


def near_shape(dims, dtype):
    return pltpu.VMEM(dims, dtype)


def call(body, out_shape, args, scratch=(), raw=(), near=(), far=()):
    spaces = [pltpu.SMEM] + [pl.ANY if i in raw else pltpu.VMEM for i in range(1, len(args))]
    args = [pltpu.with_memory_space_constraint(a, pltpu.VMEM) if i in near else a for i, a in enumerate(args)]
    args = [pltpu.with_memory_space_constraint(a, pltpu.HBM) if i in far else a for i, a in enumerate(args)]
    return pl.pallas_call(
        body,
        in_specs=[pl.BlockSpec(memory_space=m) for m in spaces],
        out_specs=[pl.BlockSpec(memory_space=pltpu.VMEM)] * len(out_shape),
        out_shape=out_shape,
        scratch_shapes=list(scratch),
        compiler_params=pltpu.CompilerParams(vmem_limit_bytes=VMEM_BYTES),
    )(*args)


def xor_move(x, axis, mask):
    return lax.ppermute(x, axis, [(i, i ^ mask) for i in range(lax.axis_size(axis))])


def doubling_gather(x, axis):
    out = x[None]
    mask = 1
    while mask < lax.axis_size(axis):
        out = jnp.concatenate([out, xor_move(out, axis, mask)], axis=0)
        mask *= 2
    return out


def halves(x):
    half = x.shape[0] // 2
    return x[:half], x[half:]


def add_low(a, b):
    return (a.astype(F32) + b.astype(F32)).astype(BF16)


def shards(samples, projections, weight_in, bias_in, weight_mid, bias_mid, weight_out, bias_out):
    n_dp, n_t = lax.axis_size("dp"), lax.axis_size("tensor")
    d, t = lax.axis_index("dp"), lax.axis_index("tensor")
    rows, patch = samples.shape
    count = projections.shape[1] // patch
    full = rows * (count + 1)
    width = weight_in.shape[1]
    part = width // n_dp
    scale = 1.0 / (rows * n_dp * count)
    half = n_t // 2
    paired = n_dp == 8 and n_t == 4
    ids = jnp.stack([t, d]).astype(jnp.int32)
    w_out = weight_out.T
    extra = 2 * patch // n_dp if paired else 0

    packs = -(-full * patch // width // 8) * 8
    send, keep, inputs = call(
        functools.partial(first_kernel, n_dp),
        [near_shape((half * full + extra, width), BF16)] * 2 + [near_shape((packs, width), BF16)],
        (ids, samples, projections, weight_in, bias_in, weight_mid),
        [pltpu.VMEM((n_t, width, width), BF16), pltpu.SemaphoreType.DMA((n_t,))],
        raw=(5,),
        far=(1, 2, 3, 4, 5),
    )

    got = xor_move(send, "tensor", 1)
    chip = [add_low(k, g) for k, g in zip(rows_of(keep, full)[:half], rows_of(got, full)[:half])]
    chip = list(lax.optimization_barrier(chip))
    hidden = [c.astype(F32) for c in chip]
    if paired:
        w_near = jnp.concatenate([keep[half * full :], got[half * full :]], axis=0)
        hidden[0] = hidden[0] + xor_move(chip[1], "tensor", 2).astype(F32)
        second = xor_move(jnp.concatenate([chip[0], w_near], axis=0), "tensor", 2)
        hidden[1] = hidden[1] + second[:full].astype(F32)
        w_far = second[full:]
    else:
        for q in range(1, half):
            for i in range(half):
                hidden[i] = hidden[i] + xor_move(chip[i ^ q], "tensor", 2 * q).astype(F32)
        sel = jnp.concatenate([weight_in, bias_in[None, :], jnp.zeros((15, width), BF16)], axis=0)
        sel = doubling_gather(lax.dynamic_slice_in_dim(sel, d * part, part, 1), "tensor")
        w_near = jnp.concatenate([sel[r] for r in range(n_t)], axis=1)
        w_far = w_near
    own = jnp.concatenate([hidden[0].astype(BF16), inputs], axis=0)
    h_keep = jnp.stack([h.astype(BF16) for h in hidden], axis=0)
    h_recv = xor_move(h_keep, "tensor", 1)

    loss, info = call(
        score_kernel,
        [shape((1, rows), F32), near_shape((rows, 2 * patch), BF16)],
        (ids, projections, h_keep, h_recv, bias_mid, w_out, bias_out),
        [pltpu.VMEM((n_t, full, patch), F32)],
        near=(2, 3, 5),
    )

    (known,) = call(
        back_kernel,
        [near_shape((patch + 16, width), BF16)],
        (ids, samples, projections, info, h_keep, h_recv, bias_mid, w_out, weight_mid, weight_in, bias_in),
        near=(3, 4, 5, 7, 8),
    )

    if paired:
        slots = {0: own}
        slots[4] = xor_move(own, "dp", 4)
        slots[2] = xor_move(own, "dp", 2)
        slots[6] = xor_move(slots[2], "dp", 4)
        for i in range(0, n_dp, 2):
            slots[i + 1] = xor_move(slots[i], "dp", 1)
        hid_parts = [jnp.stack([slots[i] for i in band]) for band in BANDS]
        edge = patch + 8
        summed, scores = known[:edge], [known[edge:]]
        for mask in (1, 2, 4):
            other = xor_move(jnp.concatenate([summed] + scores, axis=0), "dp", mask)
            last = summed, other[:edge]
            scores = scores + rows_of(other[edge:], 8)
            summed = add_low(*last)
        score_parts = [jnp.stack([scores[i] for i in band]) for band in BANDS]
    else:
        hid_parts = halves(lax.all_gather(own, "dp"))
        score_parts = halves(lax.all_gather(known[patch + 8 :], "dp"))
        summed = lax.psum(known.astype(F32), "dp")
        last = summed, jnp.zeros_like(summed)

    accs = [(n_t * part, width), (patch, width), (rows, width)]
    blocks = [near_shape((n_t, part, width), BF16), shape((patch, width), F32), shape((1, width), F32)]
    near = (1, 2, 4, 5, 6) if paired else ()
    before = ()
    for i, (hid, score) in enumerate(zip(hid_parts, score_parts)):
        final = i + 1 == len(hid_parts)
        results = call(
            functools.partial(grads_kernel, scale, n_dp, rows, full, i, final),
            blocks if final else [near_shape(dims, F32) for dims in accs],
            (ids, score, hid, bias_mid, w_out, w_near, w_far, *before),
            [pltpu.VMEM(dims, F32) for dims in accs] if final else [],
            near=near + tuple(range(7, 7 + len(before))),
        )
        before = (results[0], *before[1:], *results[1:])
    mid_block, g_out, g_mid = results

    chunks = [mid_block[0]] + [xor_move(mid_block[r], "tensor", r) for r in range(1, n_t)]
    grad_mid, g_in, g_bias_in, g_bias_out = call(
        functools.partial(merge_kernel, scale),
        [shape((part, n_t * width), F32), shape((patch, width), F32), shape((1, width), F32), shape((1, patch), F32)],
        (ids, *chunks, *last),
        near=tuple(range(1, n_t + 3)),
    )
    return (
        loss.reshape(rows),
        g_in,
        g_bias_in.reshape(width),
        grad_mid,
        g_mid.reshape(width),
        g_out.T,
        g_bias_out.reshape(patch),
    )


BANDS = (range(4), range(4, 6), range(6, 8))


def solution(mesh):
    placed = (
        P("dp", None),
        P("dp", None),
        P(None, "tensor"),
        P("tensor"),
        P("tensor", None),
        P(),
        P(),
        P(),
    )

    return jax.shard_map(
        shards,
        mesh=mesh,
        in_specs=placed,
        out_specs=(
            P("dp"),
            P(None, "tensor"),
            P("tensor"),
            P(("tensor", "dp"), None),
            P("tensor"),
            P("tensor", None),
            P(),
        ),
        check_vma=False,
    )
```

```python
import functools

import jax
import jax.numpy as jnp
from jax import lax
from jax.experimental import pallas as pl
from jax.experimental.pallas import tpu as pltpu
from jax.sharding import PartitionSpec as P


VMEM_BYTES = 16 * 2**20
F32 = jnp.float32
BF16 = jnp.bfloat16
NN = (((1,), (0,)), ((), ()))
NT = (((1,), (1,)), ((), ()))
TN = (((0,), (0,)), ((), ()))


def mm(a, b, dims):
    return lax.dot_general(a, b, dims, preferred_element_type=F32)


def stack(parts):
    return jnp.concatenate(parts, axis=0)


def swish_terms(hidden):
    gate = jax.nn.sigmoid(hidden)
    slopes = gate * (1.0 + hidden * (1.0 - gate))
    curv = gate * (1.0 - gate) * (2.0 + hidden * (1.0 - 2.0 * gate))
    return hidden * gate, slopes, curv


def rows_of(full, rows):
    count = full.shape[0] // rows
    return [full[i * rows : (i + 1) * rows] for i in range(count)]


def vectors_of(projections, patch):
    count = projections.shape[1] // patch
    return [projections[:, i * patch : (i + 1) * patch] for i in range(count)]


def input_rows(samples, projections):
    return stack([samples] + vectors_of(projections, samples.shape[1]))


def row_vector(x):
    return x.astype(F32)[None, :]


def forward_layer(pieces, bias):
    act, slopes, curv = swish_terms(pieces[0] + bias)
    layer = stack([act.astype(BF16)] + [(slopes * tan).astype(BF16) for tan in pieces[1:]])
    return layer, slopes, curv


def backward_layer(back, tans, slopes, curv):
    inner = back[1] * tans[0]
    for grad, tan in zip(back[2:], tans[1:]):
        inner = inner + grad * tan
    pre = back[0] * slopes + curv * inner
    signal = stack([pre.astype(BF16)] + [(grad * slopes).astype(BF16) for grad in back[1:]])
    return pre, signal


def pack_weights(w_in, b_in, index, n_dp):
    patch, width = w_in.shape
    part, short = width // n_dp, patch // n_dp
    row = lax.broadcasted_iota(jnp.int32, (width, part), 0)
    col = lax.broadcasted_iota(jnp.int32, (width, part), 1)
    pick = jnp.where(row == col + index * part, 1.0, 0.0).astype(BF16)
    chosen = mm(w_in, pick, NN)
    bias = mm(jnp.broadcast_to(b_in, (short, width)).astype(BF16), pick, NN)
    wide = jnp.concatenate(rows_of(chosen, short), axis=1)
    rest = jnp.concatenate([bias, jnp.zeros((short, width - part), F32)], axis=1)
    return stack([wide, rest]).astype(BF16)


def unpack_weights(packs, n_dp):
    weights, biases = [], []
    for pack in packs:
        short = pack.shape[0] // 2
        part = pack.shape[1] // n_dp
        weights.append(stack(vectors_of(pack[:short], part)))
        biases.append(pack[short : short + 1, :part])
    return jnp.concatenate(weights, axis=1).astype(BF16), jnp.concatenate(biases, axis=1)


def pack_inputs(inputs, out_rows, width):
    short = 8
    pieces = rows_of(inputs.astype(F32), short)
    wide = width // inputs.shape[1]
    pieces += [jnp.zeros_like(pieces[0])] * (out_rows // short * wide - len(pieces))
    groups = [jnp.concatenate(pieces[i : i + wide], axis=1) for i in range(0, len(pieces), wide)]
    return stack(groups).astype(BF16)


def unpack_inputs(packed, full, patch):
    short = 8
    pieces = [v for group in rows_of(packed.astype(F32), short) for v in vectors_of(group, patch)]
    return stack(pieces[: full // short]).astype(BF16)


def index_of(tile):
    return jnp.max(tile.astype(F32)).astype(jnp.int32)


def first_kernel(
    n_dp, ids, x_hbm, p_hbm, w_hbm, b_hbm, w_mid, w_out, b_mid,
    send, keep, known, inputs_out, w_buf, w_rel, b_rel, b_row, samples, projections, w_in, b_in, b_flat, sems,
):
    me = index_of(ids[0])
    width = w_in.shape[1]
    n_blocks = w_buf.shape[0]
    full = samples.shape[0] * (1 + projections.shape[1] // samples.shape[1])
    order = [*range(1, n_blocks, 2), *range(0, n_blocks, 2)]
    small = [(x_hbm, samples), (p_hbm, projections), (w_hbm, w_in), (b_hbm, b_in), (b_mid, b_flat)]
    small = [pltpu.make_async_copy(src, dst, sems.at[n_blocks + i]) for i, (src, dst) in enumerate(small)]
    for copy in small:
        copy.start()
    copies = []
    for r in order:
        cols = pl.ds(pl.multiple_of((me ^ r) * width, width), width)
        copies.append(pltpu.make_async_copy(w_mid.at[:, cols], w_buf.at[r], sems.at[r]))
        copies[-1].start()
    late = []
    for r in range(n_blocks):
        cols = pl.ds(pl.multiple_of((me ^ r) * width, width), width)
        late.append(
            pltpu.make_async_copy(
                w_out.at[:, cols], w_rel.at[:, r * width : (r + 1) * width], sems.at[n_blocks + 5 + r]
            )
        )
        late[-1].start()
    for copy in small:
        copy.wait()
    inputs = input_rows(samples[...], projections[...])
    pieces = rows_of(mm(inputs, w_in[...], NN), samples.shape[0])
    layer = forward_layer(pieces, row_vector(b_in[...]))[0]
    known[...] = pack_inputs(inputs, known.shape[0], width)
    inputs_out[...] = inputs
    b_row[...] = row_vector(b_in[...])
    for r in range(n_blocks):
        cols = pl.ds(pl.multiple_of((me ^ r) * width, width), width)
        b_rel[:, r * width : (r + 1) * width] = row_vector(b_flat[cols])
    base = n_blocks // 2 * full
    if send.shape[0] > base:
        packed = pack_weights(w_in[...], row_vector(b_in[...]), index_of(ids[1]), n_dp)
        send[base:] = packed
        keep[base:] = packed
    for r, copy in zip(order, copies):
        copy.wait()
        out = send if r % 2 else keep
        out[r // 2 * full : (r // 2 + 1) * full] = mm(layer, w_buf[r], NN).astype(BF16)
    for copy in late:
        copy.wait()


def tree_sum(parts):
    while len(parts) > 1:
        parts = [a + b for a, b in zip(parts[::2], parts[1::2])]
    return parts[0]


def score_kernel(inputs, h_keep, h_recv, b_mid, w_out, b_out, loss, info):
    width = h_keep.shape[2]
    rows = info.shape[0]
    parts = []
    for r in range(w_out.shape[1] // width):
        cols = slice(r * width, (r + 1) * width)
        h_ref = h_recv if r % 2 else h_keep
        pieces = rows_of(h_ref[r // 2].astype(F32), rows)
        layer = forward_layer(pieces, b_mid[:, cols])[0]
        parts.append(mm(layer, w_out[:, cols], NT))
    total = tree_sum(parts)
    outs = rows_of(total, rows)
    dirs = [v.astype(F32) for v in rows_of(inputs[...], rows)[1:]]
    score = outs[0] + row_vector(b_out[...])
    grad = jnp.zeros_like(score)
    losses = jnp.zeros((rows, 1), F32)
    for vec, dscore in zip(dirs, outs[1:]):
        projected = jnp.sum(vec * score, axis=1, keepdims=True)
        traced = jnp.sum(vec * dscore, axis=1, keepdims=True)
        losses = losses + traced + 0.5 * projected * projected
        grad = grad + projected * vec
    diagonal = lax.broadcasted_iota(jnp.int32, (rows, rows), 0) == lax.broadcasted_iota(jnp.int32, (rows, rows), 1)
    loss[...] = jnp.sum(jnp.where(diagonal, losses, 0.0), axis=0, keepdims=True) / len(dirs)
    high = grad.astype(BF16)
    low = (grad - high.astype(F32)).astype(BF16)
    info[...] = jnp.concatenate([high, low], axis=1)


def back_kernel(inputs, info, h_keep, h_recv, b_mid, w_out, w_mid, w_in, b_in, out):
    patch, width = w_in.shape
    rows = info.shape[0]
    inputs = inputs[...]
    out_rows = stack([info[:, :patch], inputs[rows:]])
    back_first = None
    for r in range(w_out.shape[1] // width):
        cols = slice(r * width, (r + 1) * width)
        h_ref = h_recv if r % 2 else h_keep
        pieces = rows_of(h_ref[r // 2].astype(F32), rows)
        _, slopes, curv = swish_terms(pieces[0] + b_mid[:, cols])
        back = rows_of(mm(out_rows, w_out[:, cols], NN), rows)
        signal = backward_layer(back, pieces[1:], slopes, curv)[1]
        term = mm(signal, w_mid[r], NT)
        back_first = term if back_first is None else back_first + term
    pieces = rows_of(mm(inputs, w_in[...], NN), rows)
    _, slopes, curv = swish_terms(pieces[0] + b_in[...])
    pre, signal = backward_layer(rows_of(back_first, rows), pieces[1:], slopes, curv)
    out[:patch] = mm(inputs, signal, TN).astype(BF16)
    bias = jnp.sum(pre, axis=0, keepdims=True)
    high = info[:, :patch].astype(F32)
    score = jnp.sum(high + info[:, patch:].astype(F32), axis=0, keepdims=True)
    score = jnp.concatenate([score, jnp.zeros((1, width - patch), F32)], axis=1)
    short = (out.shape[0] - patch) // 2
    wide = jnp.concatenate(rows_of(high, short), axis=1)
    wide = jnp.concatenate([wide, jnp.zeros((short, width - wide.shape[1]), F32)], axis=1)
    out[patch:] = stack([bias, score, jnp.zeros((short - 2, width), F32), wide]).astype(BF16)


def grads_kernel(scale, n_dp, rows, full, n_before, final, scores, hid, b_mid, w_out, w_near, w_far, *refs):
    count = hid.shape[0]
    before, refs = refs[: 2 * n_before + min(n_before, 1)], refs[2 * n_before + min(n_before, 1) :]
    acc, acc_out, acc_mid = refs[-3:]
    patch, width = w_out.shape[0], hid.shape[2]
    w_own = w_out[:, :width]
    b_own = b_mid[:, :width]
    paired = w_near.shape[1] == width
    if paired:
        pairs = w_near[...].astype(F32), w_far[...].astype(F32)
        w_sel, b_sel = unpack_weights([p for pair in pairs for p in rows_of(pair, pair.shape[0] // 2)], n_dp)
    else:
        w_sel, b_sel = w_near[:patch], w_near[patch : patch + 1].astype(F32)

    def terms(slot):
        inputs = unpack_inputs(hid[slot, full:], full, patch)
        groups = rows // scores.shape[1]
        score = stack(vectors_of(scores[slot].astype(F32), patch)[:groups]).astype(BF16)
        out_rows = stack([score, inputs[rows:]])
        pieces = rows_of(hid[slot, :full].astype(F32), rows)
        layer_two, slopes, curv = forward_layer(pieces, b_own)
        back = rows_of(mm(out_rows, w_own, NN), rows)
        pre, signal = backward_layer(back, pieces[1:], slopes, curv)
        layer_one = forward_layer(rows_of(mm(inputs, w_sel, NN), rows), b_sel)[0]
        return mm(layer_one, signal, TN), mm(out_rows, layer_two, TN), pre

    if paired:
        total = before[0][...] if n_before else None
        folded = None
        for step in range(0, count, 2):
            one, two = terms(step), terms(step + 1)
            total = one[0] + two[0] if total is None else total + one[0] + two[0]
            pair = one[1] + two[1], one[2] + two[2]
            folded = pair if folded is None else (folded[0] + pair[0], folded[1] + pair[1])
        acc[...] = total
        acc_out[...], acc_mid[...] = folded
    else:
        for ref in (acc, acc_out, acc_mid):
            ref[...] = jnp.zeros_like(ref)

        def body(step, carry):
            for ref, term in zip((acc, acc_out, acc_mid), terms(step)):
                ref[...] += term
            return carry

        lax.fori_loop(0, count, body, 0)
        if n_before:
            acc[...] += before[0][...]
    if not final:
        return
    block_out, g_out, g_mid = refs[:3]
    n_blocks, part = block_out.shape[0], block_out.shape[1]
    out, mid = acc_out[...], acc_mid[...]
    for i in reversed(range(n_before)):
        out = out + before[1 + 2 * i][...]
        mid = mid + before[2 + 2 * i][...]
    g_out[...] = out * scale
    g_mid[...] = jnp.sum(mid, axis=0, keepdims=True) * scale
    for r in range(n_blocks):
        block_out[r] = (acc[r * part : (r + 1) * part] * scale).astype(BF16)


def merge_kernel(scale, ids, *refs):
    me = index_of(ids[0])
    *chunks, mine, other, out, g_in, g_bias, g_last = refs
    width = mine.shape[1]
    patch = g_in.shape[0]
    for r, ref in enumerate(chunks):
        cols = pl.ds(pl.multiple_of((me ^ r) * width, width), width)
        out[:, cols] = ref[...].astype(F32)
    total = (mine[...].astype(F32) + other[...].astype(F32)) * scale
    g_in[...] = total[:patch]
    g_bias[...] = total[patch : patch + 1]
    g_last[...] = total[patch + 1 : patch + 2, :patch]


def shape(dims, dtype):
    return jax.ShapeDtypeStruct(dims, dtype)


def near_shape(dims, dtype):
    return pltpu.VMEM(dims, dtype)


def call(body, out_shape, args, scratch=(), raw=(), far=()):
    spaces = [pl.ANY if i in raw else pltpu.VMEM for i in range(len(args))]
    args = [
        pltpu.with_memory_space_constraint(a, pltpu.HBM) if i in raw
        else a if i in far
        else pltpu.with_memory_space_constraint(a, pltpu.VMEM)
        for i, a in enumerate(args)
    ]
    return pl.pallas_call(
        body,
        in_specs=[pl.BlockSpec(memory_space=m) for m in spaces],
        out_specs=[pl.BlockSpec(memory_space=pltpu.VMEM)] * len(out_shape),
        out_shape=out_shape,
        scratch_shapes=list(scratch),
        compiler_params=pltpu.CompilerParams(vmem_limit_bytes=VMEM_BYTES),
    )(*args)


def xor_move(x, axis, mask):
    return lax.ppermute(x, axis, [(i, i ^ mask) for i in range(lax.axis_size(axis))])


def doubling_gather(x, axis):
    out = x[None]
    mask = 1
    while mask < lax.axis_size(axis):
        out = jnp.concatenate([out, xor_move(out, axis, mask)], axis=0)
        mask *= 2
    return out


def halves(x):
    half = x.shape[0] // 2
    return x[:half], x[half:]


def add_low(a, b):
    return (a.astype(F32) + b.astype(F32)).astype(BF16)


def shards(samples, projections, weight_in, bias_in, weight_mid, bias_mid, weight_out, bias_out):
    n_dp, n_t = lax.axis_size("dp"), lax.axis_size("tensor")
    d, t = lax.axis_index("dp"), lax.axis_index("tensor")
    rows, patch = samples.shape
    count = projections.shape[1] // patch
    full = rows * (count + 1)
    width = weight_in.shape[1]
    part = width // n_dp
    scale = 1.0 / (rows * n_dp * count)
    half = n_t // 2
    paired = n_dp == 8 and n_t == 4
    ids = jnp.broadcast_to(jnp.stack([t, d]).astype(jnp.int32)[:, None, None], (2, 8, 128))
    w_out = weight_out.T
    extra = 2 * patch // n_dp if paired else 0

    packs = -(-full * patch // width // 8) * 8
    send, keep, packed, inputs, w_blocks, w_rel, b_rel, b_row = call(
        functools.partial(first_kernel, n_dp),
        [near_shape((half * full + extra, width), BF16)] * 2
        + [
            near_shape((packs, width), BF16),
            near_shape((full, patch), BF16),
            near_shape((n_t, width, width), BF16),
            near_shape((patch, n_t * width), BF16),
            near_shape((1, n_t * width), F32),
            near_shape((1, width), F32),
        ],
        (ids, samples, projections, weight_in, bias_in, weight_mid, w_out, bias_mid),
        [pltpu.VMEM(x.shape, BF16) for x in (samples, projections, weight_in, bias_in, bias_mid)]
        + [pltpu.SemaphoreType.DMA((2 * n_t + 5,))],
        raw=range(1, 8),
    )

    got = xor_move(send, "tensor", 1)
    chip = [add_low(k, g) for k, g in zip(rows_of(keep, full)[:half], rows_of(got, full)[:half])]
    chip = list(lax.optimization_barrier(chip))
    hidden = [c.astype(F32) for c in chip]
    if paired:
        w_near = jnp.concatenate([keep[half * full :], got[half * full :]], axis=0)
        hidden[0] = hidden[0] + xor_move(chip[1], "tensor", 2).astype(F32)
        second = xor_move(jnp.concatenate([chip[0], keep[half * full :], got[half * full :]], axis=0), "tensor", 2)
        hidden[1] = hidden[1] + second[:full].astype(F32)
        w_far = second[full:]
    else:
        for q in range(1, half):
            for i in range(half):
                hidden[i] = hidden[i] + xor_move(chip[i ^ q], "tensor", 2 * q).astype(F32)
        sel = jnp.concatenate([weight_in, bias_in[None, :], jnp.zeros((15, width), BF16)], axis=0)
        sel = doubling_gather(lax.dynamic_slice_in_dim(sel, d * part, part, 1), "tensor")
        w_near = jnp.concatenate([sel[r] for r in range(n_t)], axis=1)
        w_far = w_near
    own = jnp.concatenate([hidden[0].astype(BF16), packed], axis=0)
    h_keep = jnp.stack([h.astype(BF16) for h in hidden], axis=0)
    h_recv = xor_move(h_keep, "tensor", 1)

    loss, info = call(
        score_kernel,
        [near_shape((1, rows), F32), near_shape((rows, 2 * patch), BF16)],
        (inputs, h_keep, h_recv, b_rel, w_rel, bias_out),
    )

    (known,) = call(
        back_kernel,
        [near_shape((patch + 16, width), BF16)],
        (inputs, info, h_keep, h_recv, b_rel, w_rel, w_blocks, weight_in, b_row),
    )

    if paired:
        slots = {0: own}
        slots[4] = xor_move(own, "dp", 4)
        slots[2] = xor_move(own, "dp", 2)
        slots[6] = xor_move(slots[2], "dp", 4)
        for i in range(0, n_dp, 2):
            slots[i + 1] = xor_move(slots[i], "dp", 1)
        hid_parts = [jnp.stack([slots[i] for i in band]) for band in BANDS]
        edge = patch + 8
        summed, scores = known[:edge], [known[edge:]]
        for mask in (1, 2, 4):
            other = xor_move(jnp.concatenate([summed] + scores, axis=0), "dp", mask)
            last = summed, other[:edge]
            scores = scores + rows_of(other[edge:], 8)
            summed = add_low(*last)
        score_parts = [jnp.stack([scores[i] for i in band]) for band in BANDS]
    else:
        hid_parts = halves(lax.all_gather(own, "dp"))
        score_parts = halves(lax.all_gather(known[patch + 8 :], "dp"))
        summed = lax.psum(known.astype(F32), "dp")
        last = summed, jnp.zeros_like(summed)

    accs = [(n_t * part, width), (patch, width), (rows, width)]
    blocks = [near_shape((n_t, part, width), BF16), near_shape((patch, width), F32), near_shape((1, width), F32)]
    before = ()
    for i, (hid, score) in enumerate(zip(hid_parts, score_parts)):
        final = i + 1 == len(hid_parts)
        results = call(
            functools.partial(grads_kernel, scale, n_dp, rows, full, i, final),
            blocks if final else [near_shape(dims, F32) for dims in accs],
            (score, hid, b_rel, w_rel, w_near, w_far, *before),
            [pltpu.VMEM(dims, F32) for dims in accs] if final else [],
            far=() if paired else (0, 1),
        )
        before = (results[0], *before[1:], *results[1:])
    mid_block, g_out, g_mid = results

    chunks = [mid_block[0]] + [xor_move(mid_block[r], "tensor", r) for r in range(1, n_t)]
    grad_mid, g_in, g_bias_in, g_bias_out = call(
        functools.partial(merge_kernel, scale),
        [shape((part, n_t * width), F32), shape((patch, width), F32), shape((1, width), F32), shape((1, patch), F32)],
        (ids, *chunks, *last),
    )
    return (
        loss.reshape(rows),
        g_in,
        g_bias_in.reshape(width),
        grad_mid,
        g_mid.reshape(width),
        g_out.T,
        g_bias_out.reshape(patch),
    )


BANDS = (range(4), range(4, 6), range(6, 8))


def solution(mesh):
    placed = (
        P("dp", None),
        P("dp", None),
        P(None, "tensor"),
        P("tensor"),
        P("tensor", None),
        P(),
        P(),
        P(),
    )

    return jax.shard_map(
        shards,
        mesh=mesh,
        in_specs=placed,
        out_specs=(
            P("dp"),
            P(None, "tensor"),
            P("tensor"),
            P(("tensor", "dp"), None),
            P("tensor"),
            P("tensor", None),
            P(),
        ),
        check_vma=False,
    )
```
